32 devices in a mesh: groups: 2 (over y), batch: 8 (over z, x), heads: 2 (over core).
Axes of the slice: x: 2, y: 2, z: 4, core: 2. Of those that a mesh axis runs over, the one named last changes fastest.
Arguments:
- storage: bfloat16 [1, 4096, 4608], P(None, ('groups', 'batch', 'heads')), parts along dimension 1, may hold values from -6 to 6
- block_table: int32 [4096], P('groups'), parts along dimension 0, may hold values from 0 to 2047, as said below
- lengths: int32 [16], P(('groups', 'batch')), parts along dimension 0, may hold values from 4 to 2048
- query: bfloat16 [16, 4, 128, 576], P(('groups', 'batch'), None, 'heads'), parts along dimension 0, may hold values from -10 to 10
Outputs:
- context: bfloat16 [16, 4, 128, 512], P(('groups', 'batch'), None, 'heads'), parts along dimension 0
The draws below stay inside these ranges and needn't reach their ends.
There are 2 independent parts, one for each index of `groups`. The reference program is written for one: setup_inputs(seed, part) draws one part's arguments, and reference() takes and returns one part's arrays. A program takes and returns all parts, laid end to end along the dimension named above; each array names one. Nothing has to cross between parts.
Inputs may be any that keep to these rules, and one draw needn't show every extreme that they name: `block_table`: the entries are a permutation of 0 to 2047; entry g names block g mod 256 of sequence g // 256. Storage device k of the batch+heads order, with k = 2 b + p, holds for every batch index j exactly 16 blocks of sequences j * 1 to (j + 1) - 1, all with block numbers from p * 128 to (p + 1) * 128 - 1, in no particular order.
All inputs are finite; a program needn't handle non-finite values.
Results may differ from the reference program's by a relative error of at most 0.0031.
Values may be sent and summed in bfloat16 or wider, within the bound.
A program may use at most 64 MiB of HBM per device.

```python
import math
import jax
import jax.numpy as jnp
from jax import lax

LATENT = 512
ROPE = 64
QHEADS = 128
HEAD_NOPE = 128
SEQ_DEV = 1
MAXLEN = 2048
BLK = 8
QTOK = 4
LAYERS = 1
KVW = 576
NBLK = 256
HALF = 128
SEQS = 8
SLOTS = 2048
SLOT_DEV = 128
BLK_PEER = 16
N_BATCH = 8
N_HEADS = 2


def draw_storage(key, part):
    shape = (LAYERS, SLOTS, BLK * KVW)
    values = jnp.clip(jax.random.normal(jax.random.fold_in(key, 3), shape, jnp.float32), -4.0, 4.0)
    return values.astype(jnp.bfloat16)


def draw_query(key, part):
    shape = (SEQS, QTOK, QHEADS, KVW)
    values = jnp.clip(jax.random.normal(jax.random.fold_in(key, 5), shape, jnp.float32), -4.0, 4.0)
    return values.astype(jnp.bfloat16)


def draw_block_table(key, part):
    item_count = SEQ_DEV * HALF
    deal_keys = jax.random.split(jax.random.fold_in(key, 11), N_HEADS * N_BATCH)
    dealt = jax.vmap(lambda single: jax.random.permutation(single, item_count))(deal_keys)
    dealt = dealt.reshape(N_HEADS, N_BATCH, item_count).astype(jnp.int32)
    half_index = jnp.arange(N_HEADS, dtype=jnp.int32)[:, None, None]
    owner_index = jnp.arange(N_BATCH, dtype=jnp.int32)[None, :, None]
    sequence = owner_index * SEQ_DEV + dealt // HALF
    block = half_index * HALF + dealt % HALF
    labels = (sequence * NBLK + block).reshape(N_HEADS, N_BATCH, N_BATCH, BLK_PEER)
    labels = jnp.transpose(labels, (2, 0, 1, 3)).reshape(N_BATCH * N_HEADS, SLOT_DEV)
    shuffle_keys = jax.random.split(jax.random.fold_in(key, 13), N_BATCH * N_HEADS)
    shuffles = jax.vmap(lambda single: jax.random.permutation(single, SLOT_DEV))(shuffle_keys).astype(jnp.int32)
    labels = jnp.take_along_axis(labels, shuffles, axis=1)
    return labels.reshape(SLOTS).astype(jnp.int32)


def set_ends(entries, rng, smallest, high):
    longest = entries.shape.index(max(entries.shape))
    spots = []
    for shift in (0, 1):
        where = [jax.random.randint(jax.random.fold_in(rng, axis), (), 0, length) for axis, length in enumerate(entries.shape)]
        where[longest] = (where[longest] + shift) % entries.shape[longest]
        spots.append(tuple(where))
    return entries.at[spots[0]].set(smallest).at[spots[1]].set(high)


def setup_inputs(seed: int = 0, part: int = 0) -> dict:
    seeds = jax.random.split(jax.random.key(seed), 5)
    part_splits = jax.random.split(jax.random.fold_in(seeds[4], part), 5)
    storage = draw_storage(jax.random.fold_in(jax.random.fold_in(seeds[4], part), 71), part)
    block_table = draw_block_table(jax.random.fold_in(jax.random.fold_in(seeds[4], part), 71), part)
    lengths = set_ends(jax.random.randint(part_splits[2], (SEQS,), QTOK, MAXLEN + 1), jax.random.fold_in(part_splits[2], 1), QTOK, MAXLEN).astype(jnp.int32)
    query = draw_query(jax.random.fold_in(jax.random.fold_in(seeds[4], part), 71), part)
    return {"storage": storage, "block_table": block_table, "lengths": lengths, "query": query}


def reference(storage, block_table, lengths, query):
    slot_total = block_table.shape[0]
    inverse = jnp.zeros((slot_total,), jnp.int32).at[block_table].set(jnp.arange(slot_total, dtype=jnp.int32))
    cache = jnp.take(storage[0], inverse, axis=0).reshape(SEQS, MAXLEN, KVW)
    score_scale = 1.0 / math.sqrt(HEAD_NOPE + ROPE)
    draft = jnp.arange(QTOK * QHEADS, dtype=jnp.int32) // QHEADS
    places = jnp.arange(MAXLEN, dtype=jnp.int32)

    def one_sequence(packed):
        key_rows, query_rows, length = packed
        flat = query_rows.reshape(QTOK * QHEADS, KVW)
        scores = jnp.dot(flat, key_rows.T, preferred_element_type=jnp.float32) * score_scale
        limit = length - QTOK + draft
        visible = places[None, :] <= limit[:, None]
        masked = jnp.where(visible, scores, -1e+30)
        peak = lax.optimization_barrier(jnp.max(masked, axis=1, keepdims=True))
        raised = jnp.where(visible, jnp.exp(masked - peak), 0.0)
        totals = lax.optimization_barrier(jnp.sum(raised, axis=1, keepdims=True))
        mixed = jnp.dot(raised.astype(jnp.bfloat16), key_rows[:, :LATENT], preferred_element_type=jnp.float32)
        return (mixed / totals).astype(jnp.bfloat16).reshape(QTOK, QHEADS, LATENT)
    return lax.map(one_sequence, (cache, query, lengths))
```

```python
import functools
import math

import jax
import jax.numpy as jnp
from jax import lax
from jax.experimental import pallas as pl
from jax.experimental.pallas import tpu as pltpu
from jax.sharding import PartitionSpec as P

MESH = pl.DeviceIdType.MESH
NT = (((1,), (1,)), ((), ()))
LATENT = 512
ROPE = 64
HEAD_NOPE = 128
SEQ_DEV = 1
MAXLEN = 2048
BLK = 8
QTOK = 4


def partial_softmax(query_rows, key_rows, first_place, limits, score_scale):
    scores = (
        jnp.einsum("src,stc->srt", query_rows, key_rows, preferred_element_type=jnp.float32)
        * score_scale
    )
    places = first_place + jnp.arange(key_rows.shape[1], dtype=jnp.int32)
    visible = places[None, None, :] <= limits[:, :, None]
    masked = jnp.where(visible, scores, -1e30)
    highest = jnp.max(masked, axis=2)
    raised = jnp.where(visible, jnp.exp(masked - highest[:, :, None]), 0.0)
    totals = jnp.sum(raised, axis=2)
    mixed = jnp.einsum(
        "srt,stc->src",
        raised.astype(jnp.bfloat16),
        key_rows[:, :, :LATENT],
        preferred_element_type=jnp.float32,
    )
    return (highest, totals, mixed)


def plain_local(storage, block_table, lengths, query):
    batch_count = lax.axis_size("batch")
    head_groups = lax.axis_size("heads")
    my_batch = lax.axis_index("batch")
    my_half = lax.axis_index("heads")
    slot_count = storage.shape[1]
    per_peer = slot_count // batch_count
    block_count = MAXLEN // BLK
    half_blocks = block_count // head_groups
    width = LATENT + ROPE
    zero_index = jnp.zeros((), jnp.int32)
    table_grid = block_table.reshape(batch_count, head_groups, slot_count)
    own_table = lax.dynamic_slice(
        table_grid, (my_batch, my_half, zero_index), (1, 1, slot_count)
    ).reshape(slot_count)
    owner = own_table // block_count // SEQ_DEV
    owner_table = (owner[:, None] == jnp.arange(batch_count, dtype=jnp.int32)[None, :]).astype(
        jnp.int32
    )
    rank = jnp.sum(owner_table * (jnp.cumsum(owner_table, axis=0) - 1), axis=1)
    send_place = owner * per_peer + rank
    order = (
        jnp.zeros((slot_count,), jnp.int32)
        .at[send_place]
        .set(jnp.arange(slot_count, dtype=jnp.int32))
    )
    outgoing = jnp.take(storage, order, axis=1)
    received = lax.all_to_all(outgoing, "batch", split_axis=1, concat_axis=1, tiled=True)
    sender_table = lax.dynamic_slice(
        table_grid, (zero_index, my_half, zero_index), (batch_count, 1, slot_count)
    ).reshape(batch_count, slot_count)
    sequence_ids = sender_table // block_count
    arrivals = sequence_ids // SEQ_DEV == my_batch
    arrive_place = (
        jnp.arange(batch_count, dtype=jnp.int32)[:, None] * per_peer
        + jnp.cumsum(arrivals.astype(jnp.int32), axis=1)
        - 1
    )
    target = (
        (sequence_ids - my_batch * SEQ_DEV) * half_blocks
        + sender_table % block_count
        - my_half * half_blocks
    )
    target = jnp.where(arrivals, target, slot_count)
    source = (
        jnp.zeros((slot_count,), jnp.int32)
        .at[target.reshape(-1)]
        .set(arrive_place.reshape(-1), mode="drop")
    )
    serving = jnp.take(received, source, axis=1)
    half_length = half_blocks * BLK
    seq_count = query.shape[0]
    local_keys = serving[0].reshape(seq_count, half_length * width)
    score_scale = 1.0 / math.sqrt(HEAD_NOPE + ROPE)
    every_query = lax.all_gather(query, "heads", axis=2, tiled=True)
    all_heads = every_query.shape[2]
    row_count = QTOK * all_heads
    query_rows = every_query.reshape(seq_count, row_count, width)
    draft = jnp.arange(row_count, dtype=jnp.int32) // all_heads
    limits = lengths[:, None] - QTOK + draft[None, :]
    key_rows = local_keys.reshape(seq_count, half_length, width)
    highest, totals, mixed = partial_softmax(
        query_rows, key_rows, my_half * half_length, limits, score_scale
    )
    shaped = (
        highest.reshape(1, seq_count, QTOK, all_heads),
        totals.reshape(1, seq_count, QTOK, all_heads),
        mixed.reshape(1, seq_count, QTOK, all_heads, LATENT),
    )
    pieces = (
        lax.all_to_all(shaped[0], "heads", split_axis=3, concat_axis=0, tiled=True),
        lax.all_to_all(shaped[1], "heads", split_axis=3, concat_axis=0, tiled=True),
        lax.all_to_all(shaped[2], "heads", split_axis=3, concat_axis=0, tiled=True),
    )
    overall = jnp.max(pieces[0], axis=0)
    factor = jnp.exp(pieces[0] - overall[None])
    totals = jnp.sum(pieces[1] * factor, axis=0)
    mixed = jnp.sum(pieces[2] * factor[..., None], axis=0)
    context = (mixed / totals[..., None]).astype(jnp.bfloat16)
    return context


def fused_kernel(
    batch_count, table_ref, length_ref, storage_ref, query_ref, out_ref,
    stored, asked, outgoing, keys, query_even, query_odd,
    load_sem, send_sem, recv_sem, pass_sem, take_sem,
):
    slot_count = stored.shape[0]
    per_peer = slot_count // batch_count
    block_count = MAXLEN // BLK
    width = LATENT + ROPE
    wide = query_even.shape[1]
    me = lax.axis_index("batch")
    half = lax.axis_index("heads")
    sibling = 1 - half

    def partner(step):
        other = me
        bit = 1
        while bit < batch_count:
            if step & bit:
                other = other + bit * (1 - 2 * ((me // bit) % 2))
            bit *= 2
        return other

    load_storage = pltpu.make_async_copy(storage_ref, stored, load_sem.at[0])
    load_query = pltpu.make_async_copy(query_ref, asked, load_sem.at[1])
    load_storage.start()
    load_query.start()
    barrier = pltpu.get_barrier_semaphore()
    for step in range(1, batch_count):
        pl.semaphore_signal(
            barrier, inc=1, device_id={"batch": partner(step)}, device_id_type=MESH
        )
    pl.semaphore_signal(barrier, inc=1, device_id={"heads": sibling}, device_id_type=MESH)

    table = table_ref[...]
    device_count = table.shape[0]
    row_ids = lax.broadcasted_iota(jnp.int32, table.shape, 0)
    square = (slot_count, slot_count)
    down = lax.broadcasted_iota(jnp.int32, square, 0)
    across = lax.broadcasted_iota(jnp.int32, square, 1)
    earlier = (down < across).astype(jnp.float32).astype(jnp.bfloat16)
    own = jnp.sum(jnp.where(row_ids == 2 * me + half, table, 0), axis=0, keepdims=True)
    owner = own // block_count
    belongs = (row_ids == owner).astype(jnp.float32)
    counts = jnp.dot(belongs.astype(jnp.bfloat16), earlier, preferred_element_type=jnp.float32)
    rank = jnp.sum(belongs * counts, axis=0, keepdims=True).astype(jnp.int32)
    place = owner * per_peer + rank
    order = (down == place).astype(jnp.float32).astype(jnp.bfloat16)
    load_storage.wait()
    piece = 4 * 128
    for first in range(0, stored.shape[1], piece):
        outgoing[:, first : first + piece] = jnp.dot(
            order, stored[:, first : first + piece], preferred_element_type=jnp.float32
        ).astype(jnp.bfloat16)
    pl.semaphore_wait(barrier, batch_count)

    def rows(index):
        return pl.ds(pl.multiple_of(index * per_peer, per_peer), per_peer)

    def send(step):
        other = partner(step)
        return pltpu.make_async_remote_copy(
            src_ref=outgoing.at[rows(other)],
            dst_ref=keys.at[0, rows(me)],
            send_sem=send_sem.at[step],
            recv_sem=recv_sem.at[step],
            device_id={"batch": other},
            device_id_type=MESH,
        )

    def arrival(step):
        other = partner(step)
        return pltpu.make_async_remote_copy(
            src_ref=outgoing.at[rows(other)],
            dst_ref=keys.at[0, rows(other)],
            send_sem=send_sem.at[step],
            recv_sem=recv_sem.at[step],
            device_id={"batch": other},
            device_id_type=MESH,
        )

    def hand_over(step):
        other = partner(step)
        source = outgoing.at[rows(me)] if step == 0 else keys.at[0, rows(other)]
        return pltpu.make_async_remote_copy(
            src_ref=source,
            dst_ref=keys.at[1, rows(other)],
            send_sem=pass_sem.at[step],
            recv_sem=take_sem.at[step],
            device_id={"heads": sibling},
            device_id_type=MESH,
        )

    steps = list(range(batch_count - 1, 0, -1))
    for step in steps:
        send(step).start()
    hand_over(0).start()
    keep = pltpu.make_async_copy(outgoing.at[rows(me)], keys.at[0, rows(me)], load_sem.at[2])
    keep.start()

    mine = table // block_count == me
    marks = mine.astype(jnp.float32)
    ranks = jnp.dot(
        marks.astype(jnp.bfloat16), earlier, preferred_element_type=jnp.float32
    ).astype(jnp.int32)
    targets = jnp.where(mine, (row_ids // 2) * per_peer + ranks, -1)
    blocks = (table % block_count).astype(jnp.float32).astype(jnp.bfloat16)
    by_half = [jnp.zeros((1, slot_count), jnp.float32) for _ in range(2)]
    for index in range(device_count):
        pick = (down == targets[index : index + 1]).astype(jnp.float32).astype(jnp.bfloat16)
        by_half[index % 2] += lax.dot_general(
            blocks[index : index + 1], pick, NT, preferred_element_type=jnp.float32
        )
    first_half = half == 0
    numbers = jnp.concatenate(
        [
            jnp.where(first_half, by_half[0], by_half[1]),
            jnp.where(first_half, by_half[1], by_half[0]),
        ],
        axis=1,
    ).astype(jnp.int32)
    row_count = asked.shape[0]
    heads = row_count // QTOK
    draft = lax.broadcasted_iota(jnp.int32, (row_count, 1), 0) // heads
    limits = length_ref[0] - QTOK + draft

    load_query.wait()
    space = wide - width
    query_even[:, :width] = asked[...]
    query_even[:, width:] = jnp.zeros((row_count, space), jnp.bfloat16)
    query_odd[:, space:] = asked[...]
    query_odd[:, :space] = jnp.zeros((row_count, space), jnp.bfloat16)

    for step in steps:
        arrival(step).wait_recv()
        hand_over(step).start()
    keep.wait()
    for step in [0] + steps:
        hand_over(step).wait_recv()

    factor = math.log2(math.e) / math.sqrt(HEAD_NOPE + ROPE)
    both = 2 * slot_count
    scores = []
    for i in range(BLK):
        low = i * width // 128 * 128
        queries = query_odd if i % 2 else query_even
        part = keys[:, :, low : low + wide].reshape(both, wide)
        dots = lax.dot_general(queries[...], part, NT, preferred_element_type=jnp.float32)
        visible = numbers * BLK + i <= limits
        scores.append(jnp.where(visible, dots, -1e30))
    peak = functools.reduce(jnp.maximum, scores)
    peak = jnp.max(peak, axis=1, keepdims=True)
    totals = jnp.zeros((row_count, both), jnp.float32)
    mixed_even = jnp.zeros((row_count, LATENT), jnp.float32)
    mixed_odd = jnp.zeros((row_count, wide), jnp.float32)
    for i in range(BLK):
        low = i * width // 128 * 128
        raised = jnp.exp2((scores[i] - peak) * factor)
        totals += raised
        weights = raised.astype(jnp.bfloat16)
        if i % 2:
            part = keys[:, :, low : low + wide].reshape(both, wide)
            mixed_odd += jnp.dot(weights, part, preferred_element_type=jnp.float32)
        else:
            part = keys[:, :, low : low + LATENT].reshape(both, LATENT)
            mixed_even += jnp.dot(weights, part, preferred_element_type=jnp.float32)
    total = jnp.sum(totals, axis=1, keepdims=True)
    mixed = mixed_even + mixed_odd[:, space : space + LATENT]
    out_ref[...] = (mixed / total).astype(out_ref.dtype)
    for step in steps:
        send(step).wait_send()
    for step in [0] + steps:
        hand_over(step).wait_send()


def local(storage, block_table, lengths, query):
    batch_count = lax.axis_size("batch")
    slot_count = storage.shape[1]
    per_peer = slot_count // batch_count
    whole = batch_count & (batch_count - 1) == 0 and query.shape[0] == SEQ_DEV
    if per_peer % 16 or slot_count % 128 or not whole:
        return plain_local(storage, block_table, lengths, query)
    width = LATENT + ROPE
    heads = query.shape[2]
    row_count = QTOK * heads
    wide = -(-width // 128) * 128
    vmem = pl.BlockSpec(memory_space=pltpu.VMEM)
    anywhere = pl.BlockSpec(memory_space=pl.ANY)
    context = pl.pallas_call(
        functools.partial(fused_kernel, batch_count),
        out_shape=jax.ShapeDtypeStruct((row_count, LATENT), jnp.bfloat16),
        in_specs=[vmem, pl.BlockSpec(memory_space=pltpu.SMEM), anywhere, anywhere],
        out_specs=vmem,
        scratch_shapes=[
            pltpu.VMEM((slot_count, BLK * width), jnp.bfloat16),
            pltpu.VMEM((row_count, width), jnp.bfloat16),
            pltpu.VMEM((slot_count, BLK * width), jnp.bfloat16),
            pltpu.VMEM((2, slot_count, BLK * width), jnp.bfloat16),
            pltpu.VMEM((row_count, wide), jnp.bfloat16),
            pltpu.VMEM((row_count, wide), jnp.bfloat16),
            pltpu.SemaphoreType.DMA((3,)),
            pltpu.SemaphoreType.DMA((batch_count,)),
            pltpu.SemaphoreType.DMA((batch_count,)),
            pltpu.SemaphoreType.DMA((batch_count,)),
            pltpu.SemaphoreType.DMA((batch_count,)),
        ],
        compiler_params=pltpu.CompilerParams(collective_id=0, has_side_effects=True),
    )(
        block_table.reshape(-1, slot_count),
        lengths,
        storage[0],
        query.reshape(row_count, width),
    )
    return context.reshape(1, QTOK, heads, LATENT)


def solution(mesh):
    in_specs = (
        P(None, ("groups", "batch", "heads"), None),
        P("groups"),
        P(("groups", "batch")),
        P(("groups", "batch"), None, "heads", None),
    )
    out_specs = P(("groups", "batch"), None, "heads", None)
    return jax.shard_map(local, mesh=mesh, in_specs=in_specs, out_specs=out_specs, check_vma=False)
```

```python
import functools
import math

import jax
import jax.numpy as jnp
from jax import lax
from jax.experimental import pallas as pl
from jax.experimental.pallas import tpu as pltpu
from jax.sharding import PartitionSpec as P

MESH = pl.DeviceIdType.MESH
NT = (((1,), (1,)), ((), ()))
LATENT = 512
ROPE = 64
HEAD_NOPE = 128
SEQ_DEV = 1
MAXLEN = 2048
BLK = 8
QTOK = 4


def partial_softmax(query_rows, key_rows, first_place, limits, score_scale):
    scores = (
        jnp.einsum("src,stc->srt", query_rows, key_rows, preferred_element_type=jnp.float32)
        * score_scale
    )
    places = first_place + jnp.arange(key_rows.shape[1], dtype=jnp.int32)
    visible = places[None, None, :] <= limits[:, :, None]
    masked = jnp.where(visible, scores, -1e30)
    highest = jnp.max(masked, axis=2)
    raised = jnp.where(visible, jnp.exp(masked - highest[:, :, None]), 0.0)
    totals = jnp.sum(raised, axis=2)
    mixed = jnp.einsum(
        "srt,stc->src",
        raised.astype(jnp.bfloat16),
        key_rows[:, :, :LATENT],
        preferred_element_type=jnp.float32,
    )
    return (highest, totals, mixed)


def plain_local(storage, block_table, lengths, query):
    batch_count = lax.axis_size("batch")
    head_groups = lax.axis_size("heads")
    my_batch = lax.axis_index("batch")
    my_half = lax.axis_index("heads")
    slot_count = storage.shape[1]
    per_peer = slot_count // batch_count
    block_count = MAXLEN // BLK
    half_blocks = block_count // head_groups
    width = LATENT + ROPE
    zero_index = jnp.zeros((), jnp.int32)
    table_grid = block_table.reshape(batch_count, head_groups, slot_count)
    own_table = lax.dynamic_slice(
        table_grid, (my_batch, my_half, zero_index), (1, 1, slot_count)
    ).reshape(slot_count)
    owner = own_table // block_count // SEQ_DEV
    owner_table = (owner[:, None] == jnp.arange(batch_count, dtype=jnp.int32)[None, :]).astype(
        jnp.int32
    )
    rank = jnp.sum(owner_table * (jnp.cumsum(owner_table, axis=0) - 1), axis=1)
    send_place = owner * per_peer + rank
    order = (
        jnp.zeros((slot_count,), jnp.int32)
        .at[send_place]
        .set(jnp.arange(slot_count, dtype=jnp.int32))
    )
    outgoing = jnp.take(storage, order, axis=1)
    received = lax.all_to_all(outgoing, "batch", split_axis=1, concat_axis=1, tiled=True)
    sender_table = lax.dynamic_slice(
        table_grid, (zero_index, my_half, zero_index), (batch_count, 1, slot_count)
    ).reshape(batch_count, slot_count)
    sequence_ids = sender_table // block_count
    arrivals = sequence_ids // SEQ_DEV == my_batch
    arrive_place = (
        jnp.arange(batch_count, dtype=jnp.int32)[:, None] * per_peer
        + jnp.cumsum(arrivals.astype(jnp.int32), axis=1)
        - 1
    )
    target = (
        (sequence_ids - my_batch * SEQ_DEV) * half_blocks
        + sender_table % block_count
        - my_half * half_blocks
    )
    target = jnp.where(arrivals, target, slot_count)
    source = (
        jnp.zeros((slot_count,), jnp.int32)
        .at[target.reshape(-1)]
        .set(arrive_place.reshape(-1), mode="drop")
    )
    serving = jnp.take(received, source, axis=1)
    half_length = half_blocks * BLK
    seq_count = query.shape[0]
    local_keys = serving[0].reshape(seq_count, half_length * width)
    score_scale = 1.0 / math.sqrt(HEAD_NOPE + ROPE)
    every_query = lax.all_gather(query, "heads", axis=2, tiled=True)
    all_heads = every_query.shape[2]
    row_count = QTOK * all_heads
    query_rows = every_query.reshape(seq_count, row_count, width)
    draft = jnp.arange(row_count, dtype=jnp.int32) // all_heads
    limits = lengths[:, None] - QTOK + draft[None, :]
    key_rows = local_keys.reshape(seq_count, half_length, width)
    highest, totals, mixed = partial_softmax(
        query_rows, key_rows, my_half * half_length, limits, score_scale
    )
    shaped = (
        highest.reshape(1, seq_count, QTOK, all_heads),
        totals.reshape(1, seq_count, QTOK, all_heads),
        mixed.reshape(1, seq_count, QTOK, all_heads, LATENT),
    )
    pieces = (
        lax.all_to_all(shaped[0], "heads", split_axis=3, concat_axis=0, tiled=True),
        lax.all_to_all(shaped[1], "heads", split_axis=3, concat_axis=0, tiled=True),
        lax.all_to_all(shaped[2], "heads", split_axis=3, concat_axis=0, tiled=True),
    )
    overall = jnp.max(pieces[0], axis=0)
    factor = jnp.exp(pieces[0] - overall[None])
    totals = jnp.sum(pieces[1] * factor, axis=0)
    mixed = jnp.sum(pieces[2] * factor[..., None], axis=0)
    context = (mixed / totals[..., None]).astype(jnp.bfloat16)
    return context


def fused_kernel(
    batch_count, table_ref, length_ref, storage_ref, query_ref, out_ref,
    tabled, lengthy, stored, asked, outgoing, keys, query_even, query_odd,
    load_sem, fetch_sem, send_sem, recv_sem, pass_sem, take_sem,
):
    slot_count = stored.shape[0]
    per_peer = slot_count // batch_count
    block_count = MAXLEN // BLK
    width = LATENT + ROPE
    wide = query_even.shape[1]
    me = lax.axis_index("batch")
    half = lax.axis_index("heads")
    sibling = 1 - half

    def partner(step):
        other = me
        bit = 1
        while bit < batch_count:
            if step & bit:
                other = other + bit * (1 - 2 * ((me // bit) % 2))
            bit *= 2
        return other

    pieces = BLK // 2
    span = 2 * width

    def columns(piece):
        return pl.ds(piece * span, span)

    load_table = pltpu.make_async_copy(table_ref, tabled, load_sem.at[0])
    load_query = pltpu.make_async_copy(query_ref, asked, load_sem.at[1])
    load_length = pltpu.make_async_copy(length_ref, lengthy, load_sem.at[2])
    fetches = [
        pltpu.make_async_copy(
            storage_ref.at[:, columns(piece)], stored.at[:, columns(piece)], fetch_sem.at[piece]
        )
        for piece in range(pieces)
    ]
    load_table.start()
    for fetch in fetches:
        fetch.start()
    barrier = pltpu.get_barrier_semaphore()
    for step in range(1, batch_count):
        pl.semaphore_signal(
            barrier, inc=1, device_id={"batch": partner(step)}, device_id_type=MESH
        )
    pl.semaphore_signal(barrier, inc=1, device_id={"heads": sibling}, device_id_type=MESH)

    load_query.start()
    load_length.start()

    load_table.wait()
    table = tabled[...]
    device_count = table.shape[0]
    row_ids = lax.broadcasted_iota(jnp.int32, table.shape, 0)
    square = (slot_count, slot_count)
    down = lax.broadcasted_iota(jnp.int32, square, 0)
    across = lax.broadcasted_iota(jnp.int32, square, 1)
    earlier = (down < across).astype(jnp.float32).astype(jnp.bfloat16)
    own = jnp.sum(jnp.where(row_ids == 2 * me + half, table, 0), axis=0, keepdims=True)
    owner = own // block_count
    belongs = (row_ids == owner).astype(jnp.float32)
    counts = jnp.dot(belongs.astype(jnp.bfloat16), earlier, preferred_element_type=jnp.float32)
    rank = jnp.sum(belongs * counts, axis=0, keepdims=True).astype(jnp.int32)
    place = owner * per_peer + rank
    order = (down == place).astype(jnp.float32).astype(jnp.bfloat16)

    def group(piece):
        fetches[piece].wait()
        outgoing[:, columns(piece)] = jnp.dot(
            order, stored[:, columns(piece)], preferred_element_type=jnp.float32
        ).astype(jnp.bfloat16)

    def rows(index):
        return pl.ds(pl.multiple_of(index * per_peer, per_peer), per_peer)

    def send(step, piece):
        other = partner(step)
        return pltpu.make_async_remote_copy(
            src_ref=outgoing.at[rows(other), columns(piece)],
            dst_ref=keys.at[0, rows(me), columns(piece)],
            send_sem=send_sem.at[piece, step],
            recv_sem=recv_sem.at[piece, step],
            device_id={"batch": other},
            device_id_type=MESH,
        )

    def arrival(step, piece):
        other = partner(step)
        return pltpu.make_async_remote_copy(
            src_ref=outgoing.at[rows(other), columns(piece)],
            dst_ref=keys.at[0, rows(other), columns(piece)],
            send_sem=send_sem.at[piece, step],
            recv_sem=recv_sem.at[piece, step],
            device_id={"batch": other},
            device_id_type=MESH,
        )

    def hand_over(step, piece):
        other = partner(step)
        source = outgoing if step == 0 else keys.at[0]
        return pltpu.make_async_remote_copy(
            src_ref=source.at[rows(other), columns(piece)],
            dst_ref=keys.at[1, rows(other), columns(piece)],
            send_sem=pass_sem.at[piece, step],
            recv_sem=take_sem.at[piece, step],
            device_id={"heads": sibling},
            device_id_type=MESH,
        )

    steps = list(range(1, batch_count))

    def send_all(piece):
        for step in steps:
            send(step, piece).start()

    group(0)
    pl.semaphore_wait(barrier, batch_count)
    send_all(0)
    for piece in range(1, pieces):
        group(piece)
        if piece > 1:
            send_all(piece - 1)
    mine = table // block_count == me
    marks = mine.astype(jnp.float32)
    ranks = jnp.dot(
        marks.astype(jnp.bfloat16), earlier, preferred_element_type=jnp.float32
    ).astype(jnp.int32)
    targets = jnp.where(mine, (row_ids // 2) * per_peer + ranks, -1)
    blocks = (table % block_count).astype(jnp.float32).astype(jnp.bfloat16)
    by_half = [jnp.zeros((1, slot_count), jnp.float32) for _ in range(2)]
    for index in range(device_count):
        pick = (down == targets[index : index + 1]).astype(jnp.float32).astype(jnp.bfloat16)
        by_half[index % 2] += lax.dot_general(
            blocks[index : index + 1], pick, NT, preferred_element_type=jnp.float32
        )
    first_half = half == 0
    numbers = jnp.concatenate(
        [
            jnp.where(first_half, by_half[0], by_half[1]),
            jnp.where(first_half, by_half[1], by_half[0]),
        ],
        axis=1,
    ).astype(jnp.int32)
    for piece in range(pieces):
        hand_over(0, piece).start()
    keep = pltpu.make_async_copy(outgoing.at[rows(me)], keys.at[0, rows(me)], load_sem.at[3])
    keep.start()
    send_all(pieces - 1)

    row_count = asked.shape[0]
    heads = row_count // QTOK
    draft = lax.broadcasted_iota(jnp.int32, (row_count, 1), 0) // heads
    load_length.wait()
    limits = lengthy[0] - QTOK + draft

    load_query.wait()
    space = wide - width
    query_even[:, :width] = asked[...]
    query_even[:, width:] = jnp.zeros((row_count, space), jnp.bfloat16)
    query_odd[:, space:] = asked[...]
    query_odd[:, :space] = jnp.zeros((row_count, space), jnp.bfloat16)

    keep.wait()
    factor = math.log2(math.e) / math.sqrt(HEAD_NOPE + ROPE)
    both = 2 * slot_count
    shifted = width // 128 * 128
    peak = jnp.full((row_count, 1), -1e30, jnp.float32)
    totals = jnp.zeros((row_count, both), jnp.float32)
    mixed_even = jnp.zeros((row_count, LATENT), jnp.float32)
    mixed_odd = jnp.zeros((row_count, wide), jnp.float32)
    for piece in range(pieces):
        for step in steps:
            arrival(step, piece).wait_recv()
            hand_over(step, piece).start()
        for step in [0] + steps:
            hand_over(step, piece).wait_recv()
        base = piece * span
        parts = [
            keys[:, :, low : low + wide].reshape(both, wide) for low in (base, base + shifted)
        ]
        scores = []
        for i, queries in enumerate((query_even, query_odd)):
            dots = lax.dot_general(queries[...], parts[i], NT, preferred_element_type=jnp.float32)
            visible = numbers * BLK + (2 * piece + i) <= limits
            scores.append(jnp.where(visible, dots, -1e30))
        higher = jnp.max(jnp.maximum(scores[0], scores[1]), axis=1, keepdims=True)
        higher = jnp.maximum(peak, higher)
        shrink = jnp.exp2((peak - higher) * factor)
        peak = higher
        raised = [jnp.exp2((one - peak) * factor) for one in scores]
        totals = totals * shrink + (raised[0] + raised[1])
        mixed_even = mixed_even * shrink + jnp.dot(
            raised[0].astype(jnp.bfloat16), parts[0][:, :LATENT], preferred_element_type=jnp.float32
        )
        mixed_odd = mixed_odd * shrink + jnp.dot(
            raised[1].astype(jnp.bfloat16), parts[1], preferred_element_type=jnp.float32
        )
    total = jnp.sum(totals, axis=1, keepdims=True)
    mixed = mixed_even + mixed_odd[:, space : space + LATENT]
    out_ref[...] = (mixed / total).astype(out_ref.dtype)
    for piece in range(pieces):
        for step in steps:
            send(step, piece).wait_send()
        for step in [0] + steps:
            hand_over(step, piece).wait_send()


def local(storage, block_table, lengths, query):
    batch_count = lax.axis_size("batch")
    slot_count = storage.shape[1]
    per_peer = slot_count // batch_count
    whole = batch_count & (batch_count - 1) == 0 and query.shape[0] == SEQ_DEV
    if per_peer % 16 or slot_count % 128 or not whole:
        return plain_local(storage, block_table, lengths, query)
    width = LATENT + ROPE
    heads = query.shape[2]
    row_count = QTOK * heads
    wide = -(-width // 128) * 128
    vmem = pl.BlockSpec(memory_space=pltpu.VMEM)
    anywhere = pl.BlockSpec(memory_space=pl.ANY)
    context = pl.pallas_call(
        functools.partial(fused_kernel, batch_count),
        out_shape=jax.ShapeDtypeStruct((row_count, LATENT), jnp.bfloat16),
        in_specs=[anywhere] * 4,
        out_specs=vmem,
        scratch_shapes=[
            pltpu.VMEM((block_table.shape[0] // slot_count, slot_count), jnp.int32),
            pltpu.SMEM(lengths.shape, jnp.int32),
            pltpu.VMEM((slot_count, BLK * width), jnp.bfloat16),
            pltpu.VMEM((row_count, width), jnp.bfloat16),
            pltpu.VMEM((slot_count, BLK * width), jnp.bfloat16),
            pltpu.VMEM((2, slot_count, BLK * width), jnp.bfloat16),
            pltpu.VMEM((row_count, wide), jnp.bfloat16),
            pltpu.VMEM((row_count, wide), jnp.bfloat16),
            pltpu.SemaphoreType.DMA((4,)),
            pltpu.SemaphoreType.DMA((BLK // 2,)),
            pltpu.SemaphoreType.DMA((BLK // 2, batch_count)),
            pltpu.SemaphoreType.DMA((BLK // 2, batch_count)),
            pltpu.SemaphoreType.DMA((BLK // 2, batch_count)),
            pltpu.SemaphoreType.DMA((BLK // 2, batch_count)),
        ],
        compiler_params=pltpu.CompilerParams(collective_id=0, has_side_effects=True),
    )(
        block_table.reshape(-1, slot_count),
        lengths,
        storage[0],
        query.reshape(row_count, width),
    )
    return context.reshape(1, QTOK, heads, LATENT)


def solution(mesh):
    in_specs = (
        P(None, ("groups", "batch", "heads"), None),
        P("groups"),
        P(("groups", "batch")),
        P(("groups", "batch"), None, "heads", None),
    )
    out_specs = P(("groups", "batch"), None, "heads", None)
    return jax.shard_map(local, mesh=mesh, in_specs=in_specs, out_specs=out_specs, check_vma=False)
```

```python
import functools
import math

import jax
import jax.numpy as jnp
from jax import lax
from jax.experimental import pallas as pl
from jax.experimental.pallas import tpu as pltpu
from jax.sharding import PartitionSpec as P

MESH = pl.DeviceIdType.MESH
NT = (((1,), (1,)), ((), ()))
LATENT = 512
ROPE = 64
HEAD_NOPE = 128
SEQ_DEV = 1
MAXLEN = 2048
BLK = 8
QTOK = 4


def partial_softmax(query_rows, key_rows, first_place, limits, score_scale):
    scores = (
        jnp.einsum("src,stc->srt", query_rows, key_rows, preferred_element_type=jnp.float32)
        * score_scale
    )
    places = first_place + jnp.arange(key_rows.shape[1], dtype=jnp.int32)
    visible = places[None, None, :] <= limits[:, :, None]
    masked = jnp.where(visible, scores, -1e30)
    highest = jnp.max(masked, axis=2)
    raised = jnp.where(visible, jnp.exp(masked - highest[:, :, None]), 0.0)
    totals = jnp.sum(raised, axis=2)
    mixed = jnp.einsum(
        "srt,stc->src",
        raised.astype(jnp.bfloat16),
        key_rows[:, :, :LATENT],
        preferred_element_type=jnp.float32,
    )
    return (highest, totals, mixed)


def plain_local(storage, block_table, lengths, query):
    batch_count = lax.axis_size("batch")
    head_groups = lax.axis_size("heads")
    my_batch = lax.axis_index("batch")
    my_half = lax.axis_index("heads")
    slot_count = storage.shape[1]
    per_peer = slot_count // batch_count
    block_count = MAXLEN // BLK
    half_blocks = block_count // head_groups
    width = LATENT + ROPE
    zero_index = jnp.zeros((), jnp.int32)
    table_grid = block_table.reshape(batch_count, head_groups, slot_count)
    own_table = lax.dynamic_slice(
        table_grid, (my_batch, my_half, zero_index), (1, 1, slot_count)
    ).reshape(slot_count)
    owner = own_table // block_count // SEQ_DEV
    owner_table = (owner[:, None] == jnp.arange(batch_count, dtype=jnp.int32)[None, :]).astype(
        jnp.int32
    )
    rank = jnp.sum(owner_table * (jnp.cumsum(owner_table, axis=0) - 1), axis=1)
    send_place = owner * per_peer + rank
    order = (
        jnp.zeros((slot_count,), jnp.int32)
        .at[send_place]
        .set(jnp.arange(slot_count, dtype=jnp.int32))
    )
    outgoing = jnp.take(storage, order, axis=1)
    received = lax.all_to_all(outgoing, "batch", split_axis=1, concat_axis=1, tiled=True)
    sender_table = lax.dynamic_slice(
        table_grid, (zero_index, my_half, zero_index), (batch_count, 1, slot_count)
    ).reshape(batch_count, slot_count)
    sequence_ids = sender_table // block_count
    arrivals = sequence_ids // SEQ_DEV == my_batch
    arrive_place = (
        jnp.arange(batch_count, dtype=jnp.int32)[:, None] * per_peer
        + jnp.cumsum(arrivals.astype(jnp.int32), axis=1)
        - 1
    )
    target = (
        (sequence_ids - my_batch * SEQ_DEV) * half_blocks
        + sender_table % block_count
        - my_half * half_blocks
    )
    target = jnp.where(arrivals, target, slot_count)
    source = (
        jnp.zeros((slot_count,), jnp.int32)
        .at[target.reshape(-1)]
        .set(arrive_place.reshape(-1), mode="drop")
    )
    serving = jnp.take(received, source, axis=1)
    half_length = half_blocks * BLK
    seq_count = query.shape[0]
    local_keys = serving[0].reshape(seq_count, half_length * width)
    score_scale = 1.0 / math.sqrt(HEAD_NOPE + ROPE)
    every_query = lax.all_gather(query, "heads", axis=2, tiled=True)
    all_heads = every_query.shape[2]
    row_count = QTOK * all_heads
    query_rows = every_query.reshape(seq_count, row_count, width)
    draft = jnp.arange(row_count, dtype=jnp.int32) // all_heads
    limits = lengths[:, None] - QTOK + draft[None, :]
    key_rows = local_keys.reshape(seq_count, half_length, width)
    highest, totals, mixed = partial_softmax(
        query_rows, key_rows, my_half * half_length, limits, score_scale
    )
    shaped = (
        highest.reshape(1, seq_count, QTOK, all_heads),
        totals.reshape(1, seq_count, QTOK, all_heads),
        mixed.reshape(1, seq_count, QTOK, all_heads, LATENT),
    )
    pieces = (
        lax.all_to_all(shaped[0], "heads", split_axis=3, concat_axis=0, tiled=True),
        lax.all_to_all(shaped[1], "heads", split_axis=3, concat_axis=0, tiled=True),
        lax.all_to_all(shaped[2], "heads", split_axis=3, concat_axis=0, tiled=True),
    )
    overall = jnp.max(pieces[0], axis=0)
    factor = jnp.exp(pieces[0] - overall[None])
    totals = jnp.sum(pieces[1] * factor, axis=0)
    mixed = jnp.sum(pieces[2] * factor[..., None], axis=0)
    context = (mixed / totals[..., None]).astype(jnp.bfloat16)
    return context


def fused_kernel(
    batch_count, table_ref, length_ref, storage_ref, query_ref, out_ref,
    tabled, lengthy, stored, asked, outgoing, keys, query_even, query_odd,
    load_sem, fetch_sem, send_sem, recv_sem, pass_sem, take_sem,
):
    slot_count = stored.shape[0]
    per_peer = slot_count // batch_count
    block_count = MAXLEN // BLK
    width = LATENT + ROPE
    wide = query_even.shape[1]
    me = lax.axis_index("batch")
    half = lax.axis_index("heads")
    sibling = 1 - half

    def partner(step):
        other = me
        bit = 1
        while bit < batch_count:
            if step & bit:
                other = other + bit * (1 - 2 * ((me // bit) % 2))
            bit *= 2
        return other

    pieces = BLK // 2
    span = 2 * width

    def columns(piece):
        return pl.ds(piece * span, span)

    load_table = pltpu.make_async_copy(table_ref, tabled, load_sem.at[0])
    load_query = pltpu.make_async_copy(query_ref, asked, load_sem.at[1])
    load_length = pltpu.make_async_copy(length_ref, lengthy, load_sem.at[2])
    fetches = [
        pltpu.make_async_copy(
            storage_ref.at[:, columns(piece)], stored.at[:, columns(piece)], fetch_sem.at[piece]
        )
        for piece in range(pieces)
    ]
    load_table.start()
    for fetch in fetches:
        fetch.start()
    barrier = pltpu.get_barrier_semaphore()
    for step in range(1, batch_count):
        pl.semaphore_signal(
            barrier, inc=1, device_id={"batch": partner(step)}, device_id_type=MESH
        )
    pl.semaphore_signal(barrier, inc=1, device_id={"heads": sibling}, device_id_type=MESH)

    load_query.start()
    load_length.start()

    load_table.wait()
    table = tabled[...]
    device_count = table.shape[0]
    row_ids = lax.broadcasted_iota(jnp.int32, table.shape, 0)
    square = (slot_count, slot_count)
    down = lax.broadcasted_iota(jnp.int32, square, 0)
    across = lax.broadcasted_iota(jnp.int32, square, 1)
    earlier = (down < across).astype(jnp.float32).astype(jnp.bfloat16)
    own = jnp.sum(jnp.where(row_ids == 2 * me + half, table, 0), axis=0, keepdims=True)
    owner = own // block_count
    belongs = (row_ids == owner).astype(jnp.float32)
    counts = jnp.dot(belongs.astype(jnp.bfloat16), earlier, preferred_element_type=jnp.float32)
    rank = jnp.sum(belongs * counts, axis=0, keepdims=True).astype(jnp.int32)
    place = owner * per_peer + rank
    order = (down == place).astype(jnp.float32).astype(jnp.bfloat16)

    def group(piece):
        fetches[piece].wait()
        outgoing[:, columns(piece)] = jnp.dot(
            order, stored[:, columns(piece)], preferred_element_type=jnp.float32
        ).astype(jnp.bfloat16)

    def rows(index):
        return pl.ds(pl.multiple_of(index * per_peer, per_peer), per_peer)

    def send(step, piece):
        other = partner(step)
        return pltpu.make_async_remote_copy(
            src_ref=outgoing.at[rows(other), columns(piece)],
            dst_ref=keys.at[0, rows(me), columns(piece)],
            send_sem=send_sem.at[piece, step],
            recv_sem=recv_sem.at[piece, step],
            device_id={"batch": other},
            device_id_type=MESH,
        )

    def arrival(step, piece):
        other = partner(step)
        return pltpu.make_async_remote_copy(
            src_ref=outgoing.at[rows(other), columns(piece)],
            dst_ref=keys.at[0, rows(other), columns(piece)],
            send_sem=send_sem.at[piece, step],
            recv_sem=recv_sem.at[piece, step],
            device_id={"batch": other},
            device_id_type=MESH,
        )

    def hand_over(step, piece):
        other = partner(step)
        source = outgoing if step == 0 else keys.at[0]
        return pltpu.make_async_remote_copy(
            src_ref=source.at[rows(other), columns(piece)],
            dst_ref=keys.at[1, rows(other), columns(piece)],
            send_sem=pass_sem.at[piece, step],
            recv_sem=take_sem.at[piece, step],
            device_id={"heads": sibling},
            device_id_type=MESH,
        )

    steps = list(range(1, batch_count))

    def send_all(piece):
        for step in steps:
            send(step, piece).start()

    group(0)
    pl.semaphore_wait(barrier, batch_count)
    send_all(0)
    for piece in range(1, pieces):
        group(piece)
        if piece > 1:
            send_all(piece - 1)
    mine = table // block_count == me
    marks = mine.astype(jnp.float32)
    ranks = jnp.dot(
        marks.astype(jnp.bfloat16), earlier, preferred_element_type=jnp.float32
    ).astype(jnp.int32)
    targets = jnp.where(mine, (row_ids // 2) * per_peer + ranks, -1)
    blocks = (table % block_count).astype(jnp.float32).astype(jnp.bfloat16)
    by_half = [jnp.zeros((1, slot_count), jnp.float32) for _ in range(2)]
    for index in range(device_count):
        pick = (down == targets[index : index + 1]).astype(jnp.float32).astype(jnp.bfloat16)
        by_half[index % 2] += lax.dot_general(
            blocks[index : index + 1], pick, NT, preferred_element_type=jnp.float32
        )
    first_half = half == 0
    numbers = jnp.concatenate(
        [
            jnp.where(first_half, by_half[0], by_half[1]),
            jnp.where(first_half, by_half[1], by_half[0]),
        ],
        axis=1,
    ).astype(jnp.int32)
    for piece in range(pieces):
        hand_over(0, piece).start()
    keep = pltpu.make_async_copy(outgoing.at[rows(me)], keys.at[0, rows(me)], load_sem.at[3])
    keep.start()
    send_all(pieces - 1)

    row_count = asked.shape[0]
    heads = row_count // QTOK
    draft = lax.broadcasted_iota(jnp.int32, (row_count, 1), 0) // heads
    load_length.wait()
    limits = lengthy[0] - QTOK + draft

    load_query.wait()
    space = wide - width
    query_even[:, :width] = asked[...]
    query_even[:, width:] = jnp.zeros((row_count, space), jnp.bfloat16)
    query_odd[:, space:] = asked[...]
    query_odd[:, :space] = jnp.zeros((row_count, space), jnp.bfloat16)

    keep.wait()
    factor = math.log2(math.e) / math.sqrt(HEAD_NOPE + ROPE)
    both = 2 * slot_count
    shifted = width // 128 * 128
    peak = jnp.full((row_count, 1), -1e30, jnp.float32)
    totals = jnp.zeros((row_count, both), jnp.float32)
    mixed_even = jnp.zeros((row_count, LATENT), jnp.float32)
    mixed_odd = jnp.zeros((row_count, wide), jnp.float32)
    for piece in range(pieces):
        for step in steps:
            arrival(step, piece).wait_recv()
            hand_over(step, piece).start()
        for step in [0] + steps:
            hand_over(step, piece).wait_recv()
        base = piece * span
        parts = [
            keys[:, :, low : low + wide].reshape(both, wide) for low in (base, base + shifted)
        ]
        scores = []
        for i, queries in enumerate((query_even, query_odd)):
            dots = lax.dot_general(queries[...], parts[i], NT, preferred_element_type=jnp.float32)
            visible = numbers * BLK + (2 * piece + i) <= limits
            scores.append(jnp.where(visible, dots, -1e30))
        higher = jnp.max(jnp.maximum(scores[0], scores[1]), axis=1, keepdims=True)
        higher = jnp.maximum(peak, higher)
        shrink = jnp.exp2((peak - higher) * factor)
        peak = higher
        raised = [jnp.exp2((one - peak) * factor) for one in scores]
        totals = totals * shrink + (raised[0] + raised[1])
        mixed_even = mixed_even * shrink + jnp.dot(
            raised[0].astype(jnp.bfloat16), parts[0][:, :LATENT], preferred_element_type=jnp.float32
        )
        mixed_odd = mixed_odd * shrink + jnp.dot(
            raised[1].astype(jnp.bfloat16), parts[1], preferred_element_type=jnp.float32
        )
    total = jnp.sum(totals, axis=1, keepdims=True)
    mixed = mixed_even + mixed_odd[:, space : space + LATENT]
    out_ref[...] = (mixed / total).astype(out_ref.dtype)
    for piece in range(pieces):
        for step in steps:
            send(step, piece).wait_send()
        for step in [0] + steps:
            hand_over(step, piece).wait_send()


def local(storage, block_table, lengths, query):
    batch_count = lax.axis_size("batch")
    slot_count = storage.shape[1]
    per_peer = slot_count // batch_count
    whole = batch_count & (batch_count - 1) == 0 and query.shape[0] == SEQ_DEV
    if per_peer % 16 or slot_count % 128 or not whole:
        return plain_local(storage, block_table, lengths, query)
    width = LATENT + ROPE
    heads = query.shape[2]
    row_count = QTOK * heads
    wide = -(-width // 128) * 128
    vmem = pl.BlockSpec(memory_space=pltpu.VMEM)
    anywhere = pl.BlockSpec(memory_space=pltpu.HBM)
    context = pl.pallas_call(
        functools.partial(fused_kernel, batch_count),
        out_shape=jax.ShapeDtypeStruct((row_count, LATENT), jnp.bfloat16),
        in_specs=[anywhere] * 4,
        out_specs=vmem,
        scratch_shapes=[
            pltpu.VMEM((block_table.shape[0] // slot_count, slot_count), jnp.int32),
            pltpu.SMEM(lengths.shape, jnp.int32),
            pltpu.VMEM((slot_count, BLK * width), jnp.bfloat16),
            pltpu.VMEM((row_count, width), jnp.bfloat16),
            pltpu.VMEM((slot_count, BLK * width), jnp.bfloat16),
            pltpu.VMEM((2, slot_count, BLK * width), jnp.bfloat16),
            pltpu.VMEM((row_count, wide), jnp.bfloat16),
            pltpu.VMEM((row_count, wide), jnp.bfloat16),
            pltpu.SemaphoreType.DMA((4,)),
            pltpu.SemaphoreType.DMA((BLK // 2,)),
            pltpu.SemaphoreType.DMA((BLK // 2, batch_count)),
            pltpu.SemaphoreType.DMA((BLK // 2, batch_count)),
            pltpu.SemaphoreType.DMA((BLK // 2, batch_count)),
            pltpu.SemaphoreType.DMA((BLK // 2, batch_count)),
        ],
        compiler_params=pltpu.CompilerParams(collective_id=0, has_side_effects=True, vmem_limit_bytes=54800 * 1024),
    )(
        block_table.reshape(-1, slot_count),
        lengths,
        storage[0],
        query.reshape(row_count, width),
    )
    return context.reshape(1, QTOK, heads, LATENT)


def solution(mesh):
    in_specs = (
        P(None, ("groups", "batch", "heads"), None),
        P("groups"),
        P(("groups", "batch")),
        P(("groups", "batch"), None, "heads", None),
    )
    out_specs = P(("groups", "batch"), None, "heads", None)
    return jax.shard_map(local, mesh=mesh, in_specs=in_specs, out_specs=out_specs, check_vma=False)
```
